64 devices in a mesh: dp: 8 (over x, y, core), tp: 8 (over z).
Axes of the slice: x: 2, y: 2, z: 8, core: 2. Of those that a mesh axis runs over, the one named last changes fastest.
The devices are a block of a 4x4x8 slice.
Arguments:
- x: bfloat16 [1024, 7168], P('dp'), parts along dimension 0
- w_gate: bfloat16 [7168, 18432], P(None, 'tp')
- w_up: bfloat16 [7168, 18432], P(None, 'tp')
- w_down: bfloat16 [18432, 7168], P('tp')
Outputs:
- output: bfloat16 [1024, 7168], P('dp'), parts along dimension 0
There are 8 independent parts. The reference program is written for one: setup_inputs(seed, part) draws one part's arguments, and reference() takes and returns one part's arrays. A program takes and returns all parts, laid end to end along the dimension named above; an argument that names none is the same for every part.
All inputs are finite; a program needn't handle non-finite values.
Results may differ from the reference program's by a relative error of at most 0.016.
Values are sent between devices in bfloat16 or wider.
A program may use at most 768 MiB of HBM per device.

```python
import jax
import jax.numpy as jnp

ROWS = 128
D = 7168
FF = 18432


def setup_inputs(seed: int = 0, part: int = 0) -> dict:
    kx, kg, ku, kd = jax.random.split(jax.random.key(seed), 4)
    drawn = {
        "x": jax.random.normal(jax.random.fold_in(kx, part), (ROWS, D), jnp.float32),
        "w_gate": jax.random.normal(kg, (D, FF), jnp.float32) * D**-0.5,
        "w_up": jax.random.normal(ku, (D, FF), jnp.float32) * D**-0.5,
        "w_down": jax.random.normal(kd, (FF, D), jnp.float32) * FF**-0.5,
    }
    return {k: v.astype(jnp.bfloat16) for k, v in drawn.items()}


def reference(x, w_gate, w_up, w_down):
    gate = jnp.dot(x, w_gate, preferred_element_type=jnp.float32)
    up = jnp.dot(x, w_up, preferred_element_type=jnp.float32)
    hidden = (jax.nn.silu(gate) * up).astype(jnp.bfloat16)
    return jnp.dot(hidden, w_down, preferred_element_type=jnp.float32).astype(jnp.bfloat16)
```

```python
import functools

import jax
import jax.numpy as jnp
from jax import lax
from jax.experimental import pallas as pl
from jax.experimental.pallas import tpu as pltpu
from jax.sharding import PartitionSpec as P

F32, BF16 = jnp.float32, jnp.bfloat16
CHUNK = 512
SLOTS = 8
GROUPS = (1, 1, 2, 2, 2, 2, 2, 1, 1)
SUBS = 4


def kernel(n, x_hbm, wg_hbm, wu_hbm, wd_hbm, y_hbm, xbuf, wgu, wd, acc, hid, term, psend, precv, rsend, rrecv, y,
           x_sem, xs_sem, xr_sem, w_sem, d_sem, ps_sem, pr_sem, s_sem, r_sem, o_sem):
    rows, depth = x_hbm.shape
    share = wg_hbm.shape[1]
    part = share // 2
    cols = depth // n
    half_rows = rows // 2
    sub_rows = half_rows // SUBS
    far = n // 2
    chunks = depth // CHUNK

    dp, me = lax.axis_index("dp"), lax.axis_index("tp")
    side = lax.rem(dp, 2)
    partner = {"dp": dp + 1 - 2 * side}
    right, left = {"tp": lax.rem(me + 1, n)}, {"tp": lax.rem(me + n - 1, n)}
    to = (right, left)
    mesh_id = pl.DeviceIdType.MESH

    barrier = pltpu.get_barrier_semaphore()
    for other in (left, right, partner):
        pl.semaphore_signal(barrier, inc=1, device_id=other, device_id_type=mesh_id)

    def owner(off):
        return lax.rem(me + off + n, n)

    mine = pl.ds(pl.multiple_of(side * part, 128), part)

    def x_copy(k):
        span = pl.ds(k * CHUNK, CHUNK)
        return pltpu.make_async_copy(x_hbm.at[:, span], xbuf.at[pl.ds(0, rows), span], x_sem.at[k])

    def w_copies(k):
        src, dst = pl.ds(k * CHUNK, CHUNK), pl.ds((k % SLOTS) * CHUNK, CHUNK)
        return (
            pltpu.make_async_copy(wg_hbm.at[src, mine], wgu.at[dst, pl.ds(0, part)], w_sem.at[0, k]),
            pltpu.make_async_copy(wu_hbm.at[src, mine], wgu.at[dst, pl.ds(part, part)], w_sem.at[1, k]),
        )

    offs = [far]
    for d in range(far - 1, 0, -1):
        offs += [d, -d]
    offs.append(0)
    place = {off: i for i, off in enumerate(offs)}
    place[-far] = place[far]

    def d_copy(p):
        span = pl.ds(pl.multiple_of(owner(offs[p]) * cols, 128), cols)
        return pltpu.make_async_copy(
            wd_hbm.at[pl.ds(pl.multiple_of(side * part, 128), part), span], wd.at[p], d_sem.at[p]
        )

    for k in range(min(SLOTS, chunks)):
        x_copy(k).start()
        for c in w_copies(k):
            c.start()
    for k in range(SLOTS, chunks):
        x_copy(k).start()

    pl.semaphore_wait(barrier, 3)

    def x_send(k):
        span = pl.ds(k * CHUNK, CHUNK)
        return pltpu.make_async_remote_copy(
            x_hbm.at[:, span], xbuf.at[pl.ds(rows, rows), span], xs_sem.at[k], xr_sem.at[k],
            device_id=partner, device_id_type=mesh_id,
        )

    for k in range(chunks):
        x_send(k).start()

    k = 0
    for g, size in enumerate(GROUPS):
        for j in range(k, k + size):
            x_copy(j).wait()
            x_send(j).wait_recv()
            for c in w_copies(j):
                c.wait()
        span = pl.ds(k * CHUNK, size * CHUNK)
        slot = pl.ds((k % SLOTS) * CHUNK, size * CHUNK)
        if g < len(GROUPS) - 1:
            got = jnp.dot(xbuf[:, span], wgu[slot, :], preferred_element_type=F32)
            acc[...] = got if g == 0 else acc[...] + got
        else:
            at = 0
            while at < part:
                width = min(256, part - at)
                gs, us = pl.ds(at, width), pl.ds(part + at, width)
                gate = acc[:, gs] + jnp.dot(xbuf[:, span], wgu[slot, gs], preferred_element_type=F32)
                up = acc[:, us] + jnp.dot(xbuf[:, span], wgu[slot, us], preferred_element_type=F32)
                hid[:, gs] = (jax.nn.silu(gate) * up).astype(BF16)
                at += width
        for j in range(k, k + size):
            if j + SLOTS < chunks:
                for c in w_copies(j + SLOTS):
                    c.start()
            if j + SLOTS == chunks - 1:
                for p in range(n):
                    d_copy(p).start()
        k += size

    def p_send(p):
        return pltpu.make_async_remote_copy(
            psend.at[p], precv.at[p], ps_sem.at[p], pr_sem.at[p], device_id=partner, device_id_type=mesh_id
        )

    def down(p):
        d_copy(p).wait()
        got = jnp.dot(hid[...], wd[p], preferred_element_type=F32)
        psend[p] = got[rows:].astype(BF16)
        p_send(p).start()
        term[p] = got[:rows]

    joined = set()

    def join(p):
        if p not in joined:
            joined.add(p)
            p_send(p).wait_recv()

    def piece(h, u):
        return pl.ds(h * half_rows + u * sub_rows, sub_rows)

    def rs_step(way, t):
        h = (way + t) % 2
        return h, far - (t + 1) // 2

    def ag_step(way, t):
        return (way + t) % 2, t // 2

    hops = n - 1

    def rs_send(way, t, u):
        part_rows = pl.ds(u * sub_rows, sub_rows)
        return pltpu.make_async_remote_copy(
            rsend.at[way, t, part_rows], rrecv.at[way, t, part_rows], s_sem.at[way, t, u], r_sem.at[way, t, u],
            device_id=to[way], device_id_type=mesh_id,
        )

    def ag_ref(way, t, u, received):
        h, e = ag_step(way, t)
        e += received
        return y.at[owner(-e if way == 0 else e), piece(h, u)]

    def ag_send(way, t, u):
        ref = ag_ref(way, t, u, 0)
        return pltpu.make_async_remote_copy(
            ref, ref, s_sem.at[way, hops + t, u], r_sem.at[way, hops + t, u], device_id=to[way], device_id_type=mesh_id
        )

    def own(p, h, u):
        return term[p, piece(h, u)] + precv[p, piece(h, u)].astype(F32)

    def rs_slot(t):
        for u in range(SUBS):
            for way in range(2):
                h, d = rs_step(way, t)
                p = place[d if way == 0 else -d]
                join(p)
                total = own(p, h, u)
                if t >= 2:
                    rs_send(way, t - 2, u).wait_recv()
                    total = total + rrecv[way, t - 2, pl.ds(u * sub_rows, sub_rows)].astype(F32)
                rsend[way, t, pl.ds(u * sub_rows, sub_rows)] = total.astype(BF16)
                rs_send(way, t, u).start()

    def finish(h, u):
        p = place[0]
        join(p)
        total = own(p, h, u)
        for way in range(2):
            t = hops - 1 if rs_step(way, hops - 1)[0] == h else hops - 2
            rs_send(way, t, u).wait_recv()
            total = total + rrecv[way, t, pl.ds(u * sub_rows, sub_rows)].astype(F32)
        y[me, piece(h, u)] = total.astype(BF16)

    down(0)
    down(1)
    rs_slot(0)
    down(2)
    rs_slot(1)
    nxt = 3
    for t in range(2, hops):
        while nxt < n and (t % 2 == 0):
            down(nxt)
            nxt += 1
            if nxt % 2 == 1 and nxt < n:
                break
        rs_slot(t)
    while nxt < n:
        down(nxt)
        nxt += 1

    def out_copy(c, h):
        span = pl.ds(h * half_rows, half_rows)
        return pltpu.make_async_copy(
            y.at[c, span], y_hbm.at[span, pl.ds(pl.multiple_of(c * cols, 128), cols)], o_sem.at[c, h]
        )

    for u in range(SUBS):
        for way in range(2):
            finish(way, u)
            for w in (way, 1 - way):
                t = [t for t in range(2) if ag_step(w, t)[0] == way][0]
                ag_send(w, t, u).start()
    for h in range(2):
        out_copy(me, h).start()

    for t in range(2, hops + 2):
        for u in range(SUBS):
            for way in range(2):
                ag_send(way, t - 2, u).wait_recv()
                if t < hops:
                    ag_send(way, t, u).start()
        for way in range(2):
            h, e = ag_step(way, t)
            out_copy(owner(-e if way == 0 else e), h).start()

    for off in range(n):
        for h in range(2):
            out_copy(owner(off), h).wait()
    for k in range(chunks):
        x_send(k).wait_send()
    for p in range(n):
        p_send(p).wait_send()
    for way in range(2):
        for t in range(hops):
            for u in range(SUBS):
                rs_send(way, t, u).wait_send()
                ag_send(way, t, u).wait_send()


def solution(mesh):
    n = mesh.shape["tp"]

    def step(x, w_gate, w_up, w_down):
        rows, depth = x.shape
        share = w_gate.shape[1]
        part, cols, chunks = share // 2, depth // n, depth // CHUNK
        hops = n - 1
        dma = pltpu.SemaphoreType.DMA
        return pl.pallas_call(
            functools.partial(kernel, n),
            out_shape=jax.ShapeDtypeStruct((rows, depth), BF16),
            in_specs=[pl.BlockSpec(memory_space=pl.ANY)] * 4,
            out_specs=pl.BlockSpec(memory_space=pl.ANY),
            scratch_shapes=[
                pltpu.VMEM((2 * rows, depth), BF16),
                pltpu.VMEM((SLOTS * CHUNK, share), BF16),
                pltpu.VMEM((n, part, cols), BF16),
                pltpu.VMEM((2 * rows, share), F32),
                pltpu.VMEM((2 * rows, part), BF16),
                pltpu.VMEM((n, rows, cols), F32),
                pltpu.VMEM((n, rows, cols), BF16),
                pltpu.VMEM((n, rows, cols), BF16),
                pltpu.VMEM((2, hops, rows // 2, cols), BF16),
                pltpu.VMEM((2, hops, rows // 2, cols), BF16),
                pltpu.VMEM((n, rows, cols), BF16),
                dma((chunks,)),
                dma((chunks,)),
                dma((chunks,)),
                dma((2, chunks)),
                dma((n,)),
                dma((n,)),
                dma((n,)),
                dma((2, 2 * hops, SUBS)),
                dma((2, 2 * hops, SUBS)),
                dma((n, 2)),
            ],
            compiler_params=pltpu.CompilerParams(
                collective_id=0, has_side_effects=True, vmem_limit_bytes=67043328
            ),
        )(x, w_gate, w_up, w_down)

    return jax.shard_map(
        step,
        mesh=mesh,
        in_specs=(P("dp", None), P(None, "tp"), P(None, "tp"), P("tp", None)),
        out_specs=P("dp", None),
        check_vma=False,
    )
```

```python
import functools

import jax
import jax.numpy as jnp
from jax import lax
from jax.experimental import pallas as pl
from jax.experimental.pallas import tpu as pltpu
from jax.sharding import PartitionSpec as P

F32, BF16 = jnp.float32, jnp.bfloat16
CHUNK = 1024
SLOTS = 5
SUBS = 4
ACT_ROWS = 32


def kernel(n, x_hbm, wg_hbm, wu_hbm, wd_hbm, y, xbuf, wgu, wd, acc, hid, term, psend, precv, rsend, rrecv,
           x_sem, xs_sem, xr_sem, w_sem, d_sem, ps_sem, pr_sem, s_sem, r_sem):
    rows, depth = x_hbm.shape
    part = wg_hbm.shape[1] // 2
    cols = depth // n
    half_rows = rows // 2
    sub_rows = half_rows // SUBS
    far = n // 2
    hops = n - 1
    chunks = depth // CHUNK

    dp, me = lax.axis_index("dp"), lax.axis_index("tp")
    side = lax.rem(dp, 2)
    partner = {"dp": dp + 1 - 2 * side}
    right, left = {"tp": lax.rem(me + 1, n)}, {"tp": lax.rem(me + n - 1, n)}
    to = (right, left)
    mesh_id = pl.DeviceIdType.MESH

    barrier = pltpu.get_barrier_semaphore()
    for other in (left, right, partner):
        pl.semaphore_signal(barrier, inc=1, device_id=other, device_id_type=mesh_id)

    def owner(off):
        return lax.rem(me + off + n, n)

    mine = pl.ds(pl.multiple_of(side * part, 128), part)

    def span(k):
        return pl.ds(pl.multiple_of(k * CHUNK, CHUNK), CHUNK)

    def x_copy(k):
        return pltpu.make_async_copy(x_hbm.at[:, span(k)], xbuf.at[k, pl.ds(0, rows)], x_sem.at[k])

    def w_copies(k):
        slot = lax.rem(k, SLOTS)
        return (
            pltpu.make_async_copy(wg_hbm.at[span(k), mine], wgu.at[slot, :, pl.ds(0, part)], w_sem.at[0, k]),
            pltpu.make_async_copy(wu_hbm.at[span(k), mine], wgu.at[slot, :, pl.ds(part, part)], w_sem.at[1, k]),
        )

    def at(p):
        dist = far - (p + 1) // 2
        return owner(dist * (2 * lax.rem(p, 2) - 1))

    def d_copy(p):
        return pltpu.make_async_copy(
            wd_hbm.at[mine, pl.ds(pl.multiple_of(at(p) * cols, 128), cols)], wd.at[p], d_sem.at[p]
        )

    def start_all(*copies):
        for c in copies:
            c.start()

    def x_send(k):
        return pltpu.make_async_remote_copy(
            x_hbm.at[:, span(k)], xbuf.at[k, pl.ds(rows, rows)], xs_sem.at[k], xr_sem.at[k],
            device_id=partner, device_id_type=mesh_id,
        )

    def loop(lo, hi, body):
        def run(i, carry):
            body(i)
            return carry

        lax.fori_loop(lo, hi, run, 0)

    loop(0, SLOTS, lambda k: start_all(x_copy(k), *w_copies(k)))
    loop(SLOTS, chunks, lambda k: start_all(x_copy(k)))
    pl.semaphore_wait(barrier, 3)
    loop(0, chunks, lambda k: start_all(x_send(k)))

    def zero(r):
        acc[pl.ds(pl.multiple_of(r * 16, 16), 16)] = jnp.zeros((16, 2 * part), F32)

    loop(0, 2 * rows // 16, zero)

    def gate_up(k):
        for c in w_copies(k):
            c.wait()
        x_copy(k).wait()
        x_send(k).wait_recv()
        acc[...] += jnp.dot(xbuf[k], wgu[lax.rem(k, SLOTS)], preferred_element_type=F32)

        @pl.when(k + SLOTS < chunks)
        def _():
            start_all(*w_copies(k + SLOTS))

        @pl.when(k + SLOTS == chunks - 1)
        def _():
            loop(0, n, lambda p: start_all(d_copy(p)))

    loop(0, chunks, gate_up)

    def activate(r):
        here = pl.ds(pl.multiple_of(r * ACT_ROWS, ACT_ROWS), ACT_ROWS)
        hid[here] = (jax.nn.silu(acc[here, :part]) * acc[here, part:]).astype(BF16)

    loop(0, 2 * rows // ACT_ROWS, activate)

    def p_send(p):
        return pltpu.make_async_remote_copy(
            psend.at[p], precv.at[p], ps_sem.at[p], pr_sem.at[p], device_id=partner, device_id_type=mesh_id
        )

    def down(p):
        d_copy(p).wait()
        got = jnp.dot(hid[...], wd[p], preferred_element_type=F32)
        psend[p] = got[rows:].astype(BF16)
        p_send(p).start()
        term[p] = got[:rows]

    def piece(h, u):
        return pl.ds(pl.multiple_of(h * half_rows + u * sub_rows, sub_rows), sub_rows)

    def sub(u):
        return pl.ds(pl.multiple_of(u * sub_rows, sub_rows), sub_rows)

    def half(way, t):
        return lax.rem(way + t, 2)

    def rs_send(way, t, u):
        return pltpu.make_async_remote_copy(
            rsend.at[way, t, sub(u)], rrecv.at[way, t, sub(u)], s_sem.at[way, t, u], r_sem.at[way, t, u],
            device_id=to[way], device_id_type=mesh_id,
        )

    def ag_send(way, t, u):
        c = owner(-(t // 2) if way == 0 else t // 2)
        ref = y.at[piece(half(way, t), u), pl.ds(pl.multiple_of(c * cols, 128), cols)]
        return pltpu.make_async_remote_copy(
            ref, ref, s_sem.at[way, hops + t, u], r_sem.at[way, hops + t, u], device_id=to[way], device_id_type=mesh_id
        )

    def own(p, h, u):
        return term[p, piece(h, u)] + precv[p, piece(h, u)].astype(F32)

    def rs_place(way, t):
        first = 1 - (t + hops - 1) // hops
        p = 2 * ((t + 1) // 2)
        return p if way else p - 1 + first

    def rs_slot(t):
        @pl.when(t == 0)
        def _():
            p_send(0).wait_recv()

        @pl.when(lax.rem(t, 2) == 1)
        def _():
            p_send(t).wait_recv()
            p_send(t + 1).wait_recv()

        @pl.when(t < 2)
        def _():
            def begin(u):
                for way in range(2):
                    rsend[way, t, sub(u)] = own(rs_place(way, t), half(way, t), u).astype(BF16)
                    rs_send(way, t, u).start()

            loop(0, SUBS, begin)

        @pl.when(t >= 2)
        def _():
            def go_on(u):
                for way in range(2):
                    total = own(rs_place(way, t), half(way, t), u)
                    rs_send(way, t - 2, u).wait_recv()
                    total = total + rrecv[way, t - 2, sub(u)].astype(F32)
                    rsend[way, t, sub(u)] = total.astype(BF16)
                    rs_send(way, t, u).start()

            loop(0, SUBS, go_on)

    def down_and_ring(p):
        down(p)

        @pl.when(p >= 1)
        def _():
            rs_slot(p - 1)

    loop(0, n, down_and_ring)
    p_send(hops).wait_recv()

    mine_y = pl.ds(pl.multiple_of(me * cols, 128), cols)

    def finish(u):
        for h in range(2):
            total = own(hops, h, u)
            for way in range(2):
                t = hops - 1 if (way + hops - 1) % 2 == h else hops - 2
                rs_send(way, t, u).wait_recv()
                total = total + rrecv[way, t, sub(u)].astype(F32)
            y[piece(h, u), mine_y] = total.astype(BF16)
            for way in (h, 1 - h):
                ag_send(way, (h + way) % 2, u).start()

    loop(0, SUBS, finish)

    def forward(t):
        def one(u):
            for way in range(2):
                ag_send(way, t - 2, u).wait_recv()
                ag_send(way, t, u).start()

        loop(0, SUBS, one)

    loop(2, hops, forward)

    def last(u):
        for t in (hops - 2, hops - 1):
            for way in range(2):
                ag_send(way, t, u).wait_recv()

    loop(0, SUBS, last)

    loop(0, chunks, lambda k: x_send(k).wait_send())
    loop(0, n, lambda p: p_send(p).wait_send())

    def sent(t):
        def one(u):
            for way in range(2):
                rs_send(way, t, u).wait_send()
                ag_send(way, t, u).wait_send()

        loop(0, SUBS, one)

    loop(0, hops, sent)


def solution(mesh):
    n = mesh.shape["tp"]

    def step(x, w_gate, w_up, w_down):
        rows, depth = x.shape
        share = w_gate.shape[1]
        part, cols, chunks = share // 2, depth // n, depth // CHUNK
        hops = n - 1
        dma = pltpu.SemaphoreType.DMA
        return pl.pallas_call(
            functools.partial(kernel, n),
            out_shape=pltpu.VMEM((rows, depth), BF16),
            in_specs=[pl.BlockSpec(memory_space=pl.ANY)] * 4,
            out_specs=pl.BlockSpec(memory_space=pltpu.VMEM),
            scratch_shapes=[
                pltpu.VMEM((chunks, 2 * rows, CHUNK), BF16),
                pltpu.VMEM((SLOTS, CHUNK, share), BF16),
                pltpu.VMEM((n, part, cols), BF16),
                pltpu.VMEM((2 * rows, share), F32),
                pltpu.VMEM((2 * rows, part), BF16),
                pltpu.VMEM((n, rows, cols), F32),
                pltpu.VMEM((n, rows, cols), BF16),
                pltpu.VMEM((n, rows, cols), BF16),
                pltpu.VMEM((2, hops, rows // 2, cols), BF16),
                pltpu.VMEM((2, hops, rows // 2, cols), BF16),
                dma((chunks,)),
                dma((chunks,)),
                dma((chunks,)),
                dma((2, chunks)),
                dma((n,)),
                dma((n,)),
                dma((n,)),
                dma((2, 2 * hops, SUBS)),
                dma((2, 2 * hops, SUBS)),
            ],
            compiler_params=pltpu.CompilerParams(
                collective_id=0, has_side_effects=True, vmem_limit_bytes=62 * 1024 * 1024
            ),
        )(x, w_gate, w_up, w_down)

    return jax.shard_map(
        step,
        mesh=mesh,
        in_specs=(P("dp", None), P(None, "tp"), P(None, "tp"), P("tp", None)),
        out_specs=P("dp", None),
        check_vma=False,
    )
```

```python
import functools

import jax
import jax.numpy as jnp
from jax import lax
from jax.experimental import pallas as pl
from jax.experimental.pallas import tpu as pltpu
from jax.sharding import PartitionSpec as P

F32, BF16 = jnp.float32, jnp.bfloat16
CHUNK = 1024
SLOTS = 5
FINE = 4
COARSE = 2
ACT_ROWS = 32


def kernel(n, x_hbm, wg_hbm, wu_hbm, wd_hbm, y, xbuf, wgu, wd, acc, hid, term, psend, precv, rsend, rrecv,
           x_sem, xs_sem, xr_sem, w_sem, d_sem, ps_sem, pr_sem, s_sem, fine_sem, coarse_sem):
    rows, depth = x_hbm.shape
    part = wg_hbm.shape[1] // 2
    cols = depth // n
    half_rows = rows // 2
    far = n // 2
    hops = n - 1
    chunks = depth // CHUNK

    dp, me = lax.axis_index("dp"), lax.axis_index("tp")
    side = lax.rem(dp, 2)
    partner = {"dp": dp + 1 - 2 * side}
    right, left = {"tp": lax.rem(me + 1, n)}, {"tp": lax.rem(me + n - 1, n)}
    to = (right, left)
    mesh_id = pl.DeviceIdType.MESH

    barrier = pltpu.get_barrier_semaphore()
    for other in (left, right, partner):
        pl.semaphore_signal(barrier, inc=1, device_id=other, device_id_type=mesh_id)

    def owner(off):
        return lax.rem(me + off + n, n)

    mine = pl.ds(pl.multiple_of(side * part, 128), part)

    def span(k):
        return pl.ds(pl.multiple_of(k * CHUNK, CHUNK), CHUNK)

    x_copy = pltpu.make_async_copy(x_hbm, xbuf.at[pl.ds(0, rows)], x_sem)

    def w_copies(k):
        slot = lax.rem(k, SLOTS)
        return (
            pltpu.make_async_copy(wg_hbm.at[span(k), mine], wgu.at[slot, :, pl.ds(0, part)], w_sem.at[k]),
            pltpu.make_async_copy(wu_hbm.at[span(k), mine], wgu.at[slot, :, pl.ds(part, part)], w_sem.at[k]),
        )

    def w_wait(k):
        pltpu.make_async_copy(wg_hbm.at[span(k)], wgu.at[lax.rem(k, SLOTS)], w_sem.at[k]).wait()

    def at(p):
        dist = far - (p + 1) // 2
        return owner(dist * (2 * lax.rem(p, 2) - 1))

    def d_copy(p):
        return pltpu.make_async_copy(
            wd_hbm.at[mine, pl.ds(pl.multiple_of(at(p) * cols, 128), cols)], wd.at[p], d_sem.at[p]
        )

    def start_all(*copies):
        for c in copies:
            c.start(priority=1)

    def x_send(k):
        return pltpu.make_async_remote_copy(
            xbuf.at[pl.ds(0, rows), span(k)], xbuf.at[pl.ds(rows, rows), span(k)], xs_sem, xr_sem.at[k],
            device_id=partner, device_id_type=mesh_id,
        )

    def loop(lo, hi, body):
        def run(i, carry):
            body(i)
            return carry

        lax.fori_loop(lo, hi, run, 0)

    x_copy.start()
    loop(0, SLOTS, lambda k: start_all(*w_copies(k)))
    pl.semaphore_wait(barrier, 3)

    x_copy.wait()
    loop(0, chunks, lambda k: x_send(k).start())

    def zero(r):
        acc[pl.ds(pl.multiple_of(r * 16, 16), 16)] = jnp.zeros((16, 2 * part), F32)

    loop(0, 2 * rows // 16, zero)

    def gate_up(k):
        w_wait(k)
        x_send(k).wait_recv()
        acc[...] += jnp.dot(xbuf[:, span(k)], wgu[lax.rem(k, SLOTS)], preferred_element_type=F32)

        @pl.when(k + SLOTS < chunks)
        def _():
            start_all(*w_copies(k + SLOTS))

        @pl.when(k + SLOTS == chunks - 1)
        def _():
            loop(0, n, lambda p: start_all(d_copy(p)))

    loop(0, chunks, gate_up)

    def activate(r):
        here = pl.ds(pl.multiple_of(r * ACT_ROWS, ACT_ROWS), ACT_ROWS)
        hid[here] = (jax.nn.silu(acc[here, :part]) * acc[here, part:]).astype(BF16)

    loop(0, 2 * rows // ACT_ROWS, activate)

    def p_send(p):
        return pltpu.make_async_remote_copy(
            psend.at[p], precv.at[p], ps_sem, pr_sem.at[p], device_id=partner, device_id_type=mesh_id
        )

    def down(p):
        d_copy(p).wait()
        got = jnp.dot(hid[...], wd[p], preferred_element_type=F32)
        psend[p] = got[rows:].astype(BF16)
        p_send(p).start()
        term[p] = got[:rows]

    def half(way, t):
        return lax.rem(way + t, 2)

    def span_of(h, u, count):
        size = half_rows // count
        return pl.ds(pl.multiple_of(h * half_rows + u * size, size), size)

    def r_sem(way, slot, u, count):
        if count == FINE:
            return fine_sem.at[way, slot - (hops - 2), u]
        return coarse_sem.at[way, slot - 4 * (slot // (hops + 2)), u]

    def rs_send(way, t, u, count):
        here = span_of(0, u, count)
        return pltpu.make_async_remote_copy(
            rsend.at[way, t, here], rrecv.at[way, t, here], s_sem.at[0, way], r_sem(way, t, u, count),
            device_id=to[way], device_id_type=mesh_id,
        )

    def ag_send(way, t, u, count):
        c = owner(-(t // 2) if way == 0 else t // 2)
        ref = y.at[span_of(half(way, t), u, count), pl.ds(pl.multiple_of(c * cols, 128), cols)]
        return pltpu.make_async_remote_copy(
            ref, ref, s_sem.at[1, way], r_sem(way, hops + t, u, count), device_id=to[way], device_id_type=mesh_id
        )

    def own(p, h, u, count):
        here = span_of(h, u, count)
        return term[p, here] + precv[p, here].astype(F32)

    def rs_place(way, t):
        first = 1 - (t + hops - 1) // hops
        p = 2 * ((t + 1) // 2)
        return p if way else p - 1 + first

    def rs_slot(t):
        @pl.when(t == 0)
        def _():
            p_send(0).wait_recv()

        @pl.when(lax.rem(t, 2) == 1)
        def _():
            p_send(t).wait_recv()
            p_send(t + 1).wait_recv()

        def pass_on(way, u, count, add):
            total = own(rs_place(way, t), half(way, t), u, count)
            here = span_of(0, u, count)
            if add:
                total = total + rrecv[way, t - 2, here].astype(F32)
            rsend[way, t, here] = total.astype(BF16)
            rs_send(way, t, u, count).start()

        @pl.when(t < 2)
        def _():
            def begin(u):
                for way in range(2):
                    pass_on(way, u, COARSE, False)

            loop(0, COARSE, begin)

        @pl.when((t >= 2) & (t < hops - 2))
        def _():
            def middle(u):
                for way in range(2):
                    rs_send(way, t - 2, u, COARSE).wait_recv()
                    pass_on(way, u, COARSE, True)

            loop(0, COARSE, middle)

        @pl.when(t >= hops - 2)
        def _():
            def end(u):
                for way in range(2):
                    rs_send(way, t - 2, u, COARSE).wait_recv()
                    for v in range(FINE // COARSE):
                        pass_on(way, u * (FINE // COARSE) + v, FINE, True)

            loop(0, COARSE, end)

    def down_and_ring(p):
        down(p)

        @pl.when(p >= 1)
        def _():
            rs_slot(p - 1)

    loop(0, n, down_and_ring)
    p_send(hops).wait_recv()

    mine_y = pl.ds(pl.multiple_of(me * cols, 128), cols)

    def finish(u):
        for h in range(2):
            total = own(hops, h, u, FINE)
            for way in range(2):
                t = hops - 1 if (way + hops - 1) % 2 == h else hops - 2
                rs_send(way, t, u, FINE).wait_recv()
                total = total + rrecv[way, t, span_of(0, u, FINE)].astype(F32)
            y[span_of(h, u, FINE), mine_y] = total.astype(BF16)
            for way in (h, 1 - h):
                ag_send(way, (h + way) % 2, u, FINE).start()

    loop(0, FINE, finish)

    def forward_first(t):
        def one(u):
            for way in range(2):
                for v in range(FINE // COARSE):
                    ag_send(way, t - 2, u * (FINE // COARSE) + v, FINE).wait_recv()
                ag_send(way, t, u, COARSE).start()

        loop(0, COARSE, one)

    def forward(t):
        def one(u):
            for way in range(2):
                ag_send(way, t - 2, u, COARSE).wait_recv()
                ag_send(way, t, u, COARSE).start()

        loop(0, COARSE, one)

    loop(2, 4, forward_first)
    loop(4, hops, forward)

    def last(u):
        for t in (hops - 2, hops - 1):
            for way in range(2):
                ag_send(way, t, u, COARSE).wait_recv()

    loop(0, COARSE, last)

    pltpu.make_async_remote_copy(
        xbuf.at[pl.ds(0, rows)], xbuf.at[pl.ds(rows, rows)], xs_sem, xr_sem.at[0], device_id=partner, device_id_type=mesh_id
    ).wait_send()
    pltpu.make_async_remote_copy(
        psend, precv, ps_sem, pr_sem.at[0], device_id=partner, device_id_type=mesh_id
    ).wait_send()
    for way in range(2):
        for stage in range(2):
            pltpu.make_async_remote_copy(
                rsend.at[way], rrecv.at[way], s_sem.at[stage, way], coarse_sem.at[0, 0, 0],
                device_id=to[way], device_id_type=mesh_id,
            ).wait_send()


def solution(mesh):
    n = mesh.shape["tp"]

    def step(x, w_gate, w_up, w_down):
        rows, depth = x.shape
        share = w_gate.shape[1]
        part, cols, chunks = share // 2, depth // n, depth // CHUNK
        hops = n - 1
        dma = pltpu.SemaphoreType.DMA
        return pl.pallas_call(
            functools.partial(kernel, n),
            out_shape=pltpu.VMEM((rows, depth), BF16),
            in_specs=[pl.BlockSpec(memory_space=pl.ANY)] * 4,
            out_specs=pl.BlockSpec(memory_space=pltpu.VMEM),
            scratch_shapes=[
                pltpu.VMEM((2 * rows, depth), BF16),
                pltpu.VMEM((SLOTS, CHUNK, share), BF16),
                pltpu.VMEM((n, part, cols), BF16),
                pltpu.VMEM((2 * rows, share), F32),
                pltpu.VMEM((2 * rows, part), BF16),
                pltpu.VMEM((n, rows, cols), F32),
                pltpu.VMEM((n, rows, cols), BF16),
                pltpu.VMEM((n, rows, cols), BF16),
                pltpu.VMEM((2, hops, rows // 2, cols), BF16),
                pltpu.VMEM((2, hops, rows // 2, cols), BF16),
                dma,
                dma,
                dma((chunks,)),
                dma((chunks,)),
                dma((n,)),
                dma,
                dma((n,)),
                dma((2, 2)),
                dma((2, 4, FINE)),
                dma((2, 2 * (hops - 2), COARSE)),
            ],
            compiler_params=pltpu.CompilerParams(
                collective_id=0, has_side_effects=True, vmem_limit_bytes=62 * 1024 * 1024
            ),
        )(x, w_gate, w_up, w_down)

    return jax.shard_map(
        step,
        mesh=mesh,
        in_specs=(P("dp", None), P(None, "tp"), P(None, "tp"), P("tp", None)),
        out_specs=P("dp", None),
        check_vma=False,
    )
```

```python
import functools

import jax
import jax.numpy as jnp
from jax import lax
from jax.experimental import pallas as pl
from jax.experimental.pallas import tpu as pltpu
from jax.sharding import PartitionSpec as P

F32, BF16 = jnp.float32, jnp.bfloat16
CHUNK = 1024
SLOTS = 5
FINE = 4
COARSE = 2
ACT_ROWS = 32


def kernel(n, x_hbm, wg_hbm, wu_hbm, wd_hbm, y, xbuf, wgu, wd, acc, hid, term, psend, precv, rsend, rrecv,
           x_sem, xs_sem, xr_sem, w_sem, d_sem, ps_sem, pr_sem, s_sem, fine_sem, coarse_sem):
    rows, depth = x_hbm.shape
    part = wg_hbm.shape[1] // 2
    cols = depth // n
    half_rows = rows // 2
    far = n // 2
    hops = n - 1
    chunks = depth // CHUNK

    dp, me = lax.axis_index("dp"), lax.axis_index("tp")
    side = lax.rem(dp, 2)
    partner = {"dp": dp + 1 - 2 * side}
    right, left = {"tp": lax.rem(me + 1, n)}, {"tp": lax.rem(me + n - 1, n)}
    to = (right, left)
    mesh_id = pl.DeviceIdType.MESH

    def owner(off):
        return lax.rem(me + off + n, n)

    mine = pl.ds(pl.multiple_of(side * part, 128), part)

    def span(k):
        return pl.ds(pl.multiple_of(k * CHUNK, CHUNK), CHUNK)

    x_copy = pltpu.make_async_copy(x_hbm, xbuf.at[pl.ds(0, rows)], x_sem)

    def w_copies(k):
        slot = lax.rem(k, SLOTS)
        return (
            pltpu.make_async_copy(wg_hbm.at[span(k), mine], wgu.at[slot, :, pl.ds(0, part)], w_sem.at[k]),
            pltpu.make_async_copy(wu_hbm.at[span(k), mine], wgu.at[slot, :, pl.ds(part, part)], w_sem.at[k]),
        )

    def w_wait(k):
        pltpu.make_async_copy(wg_hbm.at[span(k)], wgu.at[lax.rem(k, SLOTS)], w_sem.at[k]).wait()

    def at(p):
        dist = far - (p + 1) // 2
        return owner(dist * (2 * lax.rem(p, 2) - 1))

    def d_copy(p):
        return pltpu.make_async_copy(
            wd_hbm.at[mine, pl.ds(pl.multiple_of(at(p) * cols, 128), cols)], wd.at[p], d_sem.at[p]
        )

    def start_all(*copies):
        for c in copies:
            c.start(priority=1)

    def x_send(k):
        return pltpu.make_async_remote_copy(
            xbuf.at[pl.ds(0, rows), span(k)], xbuf.at[pl.ds(rows, rows), span(k)], xs_sem, xr_sem.at[k],
            device_id=partner, device_id_type=mesh_id,
        )

    def loop(lo, hi, body):
        def run(i, carry):
            body(i)
            return carry

        lax.fori_loop(lo, hi, run, 0)

    x_copy.start()
    loop(0, SLOTS, lambda k: start_all(*w_copies(k)))

    barrier = pltpu.get_barrier_semaphore()
    for other in (left, right, partner):
        pl.semaphore_signal(barrier, inc=1, device_id=other, device_id_type=mesh_id)
    pl.semaphore_wait(barrier, 3)

    x_copy.wait()
    loop(0, chunks, lambda k: x_send(k).start())

    def zero(r):
        acc[pl.ds(pl.multiple_of(r * 16, 16), 16)] = jnp.zeros((16, 2 * part), F32)

    loop(0, 2 * rows // 16, zero)

    def gate_up(k):
        w_wait(k)
        x_send(k).wait_recv()
        acc[...] += jnp.dot(xbuf[:, span(k)], wgu[lax.rem(k, SLOTS)], preferred_element_type=F32)

        @pl.when(k + SLOTS < chunks)
        def _():
            start_all(*w_copies(k + SLOTS))

        @pl.when(k + SLOTS == chunks - 1)
        def _():
            loop(0, n, lambda p: start_all(d_copy(p)))

    loop(0, chunks, gate_up)

    def activate(r):
        here = pl.ds(pl.multiple_of(r * ACT_ROWS, ACT_ROWS), ACT_ROWS)
        hid[here] = (jax.nn.silu(acc[here, :part]) * acc[here, part:]).astype(BF16)

    loop(0, 2 * rows // ACT_ROWS, activate)

    def p_send(p):
        return pltpu.make_async_remote_copy(
            psend.at[p], precv.at[p], ps_sem, pr_sem.at[p], device_id=partner, device_id_type=mesh_id
        )

    def down(p):
        d_copy(p).wait()
        got = jnp.dot(hid[...], wd[p], preferred_element_type=F32)
        psend[p] = got[rows:].astype(BF16)
        p_send(p).start()
        term[p] = got[:rows]

    def half(way, t):
        return lax.rem(way + t, 2)

    def span_of(h, u, count):
        size = half_rows // count
        return pl.ds(pl.multiple_of(h * half_rows + u * size, size), size)

    def r_sem(way, slot, u, count):
        if count == FINE:
            return fine_sem.at[way, slot - (hops - 2), u]
        return coarse_sem.at[way, slot - 4 * (slot // (hops + 2)), u]

    def rs_send(way, t, u, count):
        here = span_of(0, u, count)
        return pltpu.make_async_remote_copy(
            rsend.at[way, t, here], rrecv.at[way, t, here], s_sem.at[0, way], r_sem(way, t, u, count),
            device_id=to[way], device_id_type=mesh_id,
        )

    def ag_send(way, t, u, count):
        c = owner(-(t // 2) if way == 0 else t // 2)
        ref = y.at[span_of(half(way, t), u, count), pl.ds(pl.multiple_of(c * cols, 128), cols)]
        return pltpu.make_async_remote_copy(
            ref, ref, s_sem.at[1, way], r_sem(way, hops + t, u, count), device_id=to[way], device_id_type=mesh_id
        )

    def own(p, h, u, count):
        here = span_of(h, u, count)
        return term[p, here] + precv[p, here].astype(F32)

    def rs_place(way, t):
        first = 1 - (t + hops - 1) // hops
        p = 2 * ((t + 1) // 2)
        return p if way else p - 1 + first

    def rs_slot(t):
        @pl.when(t == 0)
        def _():
            p_send(0).wait_recv()

        @pl.when(lax.rem(t, 2) == 1)
        def _():
            p_send(t).wait_recv()
            p_send(t + 1).wait_recv()

        def pass_on(way, u, count, add):
            total = own(rs_place(way, t), half(way, t), u, count)
            here = span_of(0, u, count)
            if add:
                total = total + rrecv[way, t - 2, here].astype(F32)
            rsend[way, t, here] = total.astype(BF16)
            rs_send(way, t, u, count).start()

        @pl.when(t < 2)
        def _():
            def begin(u):
                for way in range(2):
                    pass_on(way, u, COARSE, False)

            loop(0, COARSE, begin)

        @pl.when((t >= 2) & (t < hops - 2))
        def _():
            def middle(u):
                for way in range(2):
                    rs_send(way, t - 2, u, COARSE).wait_recv()
                    pass_on(way, u, COARSE, True)

            loop(0, COARSE, middle)

        @pl.when(t >= hops - 2)
        def _():
            def end(u):
                for way in range(2):
                    rs_send(way, t - 2, u, COARSE).wait_recv()
                    for v in range(FINE // COARSE):
                        pass_on(way, u * (FINE // COARSE) + v, FINE, True)

            loop(0, COARSE, end)

    def down_and_ring(p):
        @pl.when(p < n)
        def _():
            down(p)

        late = p // 6

        @pl.when(lax.rem(p, 2) + late >= 1)
        def _():
            rs_slot((1 - late) * ((p - 1) // 2) + late * (p - 3))

    loop(0, hops + 3, down_and_ring)
    p_send(hops).wait_recv()

    mine_y = pl.ds(pl.multiple_of(me * cols, 128), cols)

    def finish(u):
        for h in range(2):
            total = own(hops, h, u, FINE)
            for way in range(2):
                t = hops - 1 if (way + hops - 1) % 2 == h else hops - 2
                rs_send(way, t, u, FINE).wait_recv()
                total = total + rrecv[way, t, span_of(0, u, FINE)].astype(F32)
            y[span_of(h, u, FINE), mine_y] = total.astype(BF16)
            for way in (h, 1 - h):
                ag_send(way, (h + way) % 2, u, FINE).start()

    loop(0, FINE, finish)

    def forward_first(t):
        def one(u):
            for way in range(2):
                for v in range(FINE // COARSE):
                    ag_send(way, t - 2, u * (FINE // COARSE) + v, FINE).wait_recv()
                ag_send(way, t, u, COARSE).start()

        loop(0, COARSE, one)

    def forward(t):
        def one(u):
            for way in range(2):
                ag_send(way, t - 2, u, COARSE).wait_recv()
                ag_send(way, t, u, COARSE).start()

        loop(0, COARSE, one)

    loop(2, 4, forward_first)
    loop(4, hops, forward)

    def last(u):
        for t in (hops - 2, hops - 1):
            for way in range(2):
                ag_send(way, t, u, COARSE).wait_recv()

    loop(0, COARSE, last)

    pltpu.make_async_remote_copy(
        xbuf.at[pl.ds(0, rows)], xbuf.at[pl.ds(rows, rows)], xs_sem, xr_sem.at[0], device_id=partner, device_id_type=mesh_id
    ).wait_send()
    pltpu.make_async_remote_copy(
        psend, precv, ps_sem, pr_sem.at[0], device_id=partner, device_id_type=mesh_id
    ).wait_send()
    for way in range(2):
        for stage in range(2):
            pltpu.make_async_remote_copy(
                rsend.at[way], rrecv.at[way], s_sem.at[stage, way], coarse_sem.at[0, 0, 0],
                device_id=to[way], device_id_type=mesh_id,
            ).wait_send()


def solution(mesh):
    n = mesh.shape["tp"]

    def step(x, w_gate, w_up, w_down):
        rows, depth = x.shape
        share = w_gate.shape[1]
        part, cols, chunks = share // 2, depth // n, depth // CHUNK
        hops = n - 1
        dma = pltpu.SemaphoreType.DMA
        return pl.pallas_call(
            functools.partial(kernel, n),
            out_shape=pltpu.VMEM((rows, depth), BF16),
            in_specs=[pl.BlockSpec(memory_space=pl.ANY)] * 4,
            out_specs=pl.BlockSpec(memory_space=pltpu.VMEM),
            scratch_shapes=[
                pltpu.VMEM((2 * rows, depth), BF16),
                pltpu.VMEM((SLOTS, CHUNK, share), BF16),
                pltpu.VMEM((n, part, cols), BF16),
                pltpu.VMEM((2 * rows, share), F32),
                pltpu.VMEM((2 * rows, part), BF16),
                pltpu.VMEM((n, rows, cols), F32),
                pltpu.VMEM((n, rows, cols), BF16),
                pltpu.VMEM((n, rows, cols), BF16),
                pltpu.VMEM((2, hops, rows // 2, cols), BF16),
                pltpu.VMEM((2, hops, rows // 2, cols), BF16),
                dma,
                dma,
                dma((chunks,)),
                dma((chunks,)),
                dma((n,)),
                dma,
                dma((n,)),
                dma((2, 2)),
                dma((2, 4, FINE)),
                dma((2, 2 * (hops - 2), COARSE)),
            ],
            compiler_params=pltpu.CompilerParams(
                collective_id=0, has_side_effects=True, vmem_limit_bytes=62 * 1024 * 1024
            ),
        )(x, w_gate, w_up, w_down)

    return jax.shard_map(
        step,
        mesh=mesh,
        in_specs=(P("dp", None), P(None, "tp"), P(None, "tp"), P("tp", None)),
        out_specs=P("dp", None),
        check_vma=False,
    )
```

```python
import functools

import jax
import jax.numpy as jnp
from jax import lax
from jax.experimental import pallas as pl
from jax.experimental.pallas import tpu as pltpu
from jax.sharding import PartitionSpec as P

F32, BF16 = jnp.float32, jnp.bfloat16
CHUNK = 1024
SLOTS = 5
FINE = 4
COARSE = 2
ACT_ROWS = 32


def kernel(n, x_hbm, wg_hbm, wu_hbm, wd_hbm, y, xbuf, wgu, wd, acc, hid, term, psend, precv, rsend, rrecv,
           x_sem, xs_sem, xr_sem, w_sem, d_sem, ps_sem, pr_sem, s_sem, fine_sem, coarse_sem):
    rows, depth = x_hbm.shape
    part = wg_hbm.shape[1] // 2
    cols = depth // n
    half_rows = rows // 2
    far = n // 2
    hops = n - 1
    chunks = depth // CHUNK

    dp, me = lax.axis_index("dp"), lax.axis_index("tp")
    side = lax.rem(dp, 2)
    partner = {"dp": dp + 1 - 2 * side}
    right, left = {"tp": lax.rem(me + 1, n)}, {"tp": lax.rem(me + n - 1, n)}
    to = (right, left)
    mesh_id = pl.DeviceIdType.MESH

    def owner(off):
        return lax.rem(me + off + n, n)

    mine = pl.ds(pl.multiple_of(side * part, 128), part)

    def span(k):
        return pl.ds(pl.multiple_of(k * CHUNK, CHUNK), CHUNK)

    x_copy = pltpu.make_async_copy(x_hbm, xbuf.at[pl.ds(0, rows)], x_sem)

    def w_copies(k):
        slot = lax.rem(k, SLOTS)
        return (
            pltpu.make_async_copy(wg_hbm.at[span(k), mine], wgu.at[slot, :, pl.ds(0, part)], w_sem.at[k]),
            pltpu.make_async_copy(wu_hbm.at[span(k), mine], wgu.at[slot, :, pl.ds(part, part)], w_sem.at[k]),
        )

    def w_wait(k):
        pltpu.make_async_copy(wg_hbm.at[span(k)], wgu.at[lax.rem(k, SLOTS)], w_sem.at[k]).wait()

    def at(p):
        dist = far - (p + 1) // 2
        return owner(dist * (2 * lax.rem(p, 2) - 1))

    def d_copy(p):
        return pltpu.make_async_copy(
            wd_hbm.at[mine, pl.ds(pl.multiple_of(at(p) * cols, 128), cols)], wd.at[p], d_sem.at[p]
        )

    def start_all(*copies):
        for c in copies:
            c.start(priority=1)

    def x_send(k):
        return pltpu.make_async_remote_copy(
            xbuf.at[pl.ds(0, rows), span(k)], xbuf.at[pl.ds(rows, rows), span(k)], xs_sem, xr_sem.at[k],
            device_id=partner, device_id_type=mesh_id,
        )

    def loop(lo, hi, body):
        def run(i, carry):
            body(i)
            return carry

        lax.fori_loop(lo, hi, run, 0)

    x_copy.start()
    loop(0, SLOTS, lambda k: start_all(*w_copies(k)))

    barrier = pltpu.get_barrier_semaphore()
    for other in (left, right, partner):
        pl.semaphore_signal(barrier, inc=1, device_id=other, device_id_type=mesh_id)
    pl.semaphore_wait(barrier, 3)

    x_copy.wait()
    loop(0, chunks, lambda k: x_send(k).start())

    def zero(r):
        acc[pl.ds(pl.multiple_of(r * 16, 16), 16)] = jnp.zeros((16, 2 * part), F32)

    loop(0, 2 * rows // 16, zero)

    def gate_up(k):
        w_wait(k)
        x_send(k).wait_recv()
        acc[...] += jnp.dot(xbuf[:, span(k)], wgu[lax.rem(k, SLOTS)], preferred_element_type=F32)

        @pl.when(k + SLOTS < chunks)
        def _():
            start_all(*w_copies(k + SLOTS))

        @pl.when(k + SLOTS == chunks - 1)
        def _():
            loop(0, n, lambda p: start_all(d_copy(p)))

    loop(0, chunks, gate_up)

    def activate(r):
        here = pl.ds(pl.multiple_of(r * ACT_ROWS, ACT_ROWS), ACT_ROWS)
        hid[here] = (jax.nn.silu(acc[here, :part]) * acc[here, part:]).astype(BF16)

    loop(0, 2 * rows // ACT_ROWS, activate)

    def p_send(p):
        return pltpu.make_async_remote_copy(
            psend.at[p], precv.at[p], ps_sem, pr_sem.at[p], device_id=partner, device_id_type=mesh_id
        )

    def down(p):
        d_copy(p).wait()
        got = jnp.dot(hid[...], wd[p], preferred_element_type=F32)
        psend[p] = got[rows:].astype(BF16)
        p_send(p).start()
        term[p] = got[:rows]

    def half(way, t):
        return lax.rem(way + t, 2)

    def span_of(h, u, count):
        size = half_rows // count
        return pl.ds(pl.multiple_of(h * half_rows + u * size, size), size)

    def r_sem(way, slot, u, count):
        if count == FINE:
            return fine_sem.at[way, slot - (hops - 2), u]
        return coarse_sem.at[way, slot - (hops + 2) * (slot // (hops + 2)), u]

    def rs_send(way, t, u, count):
        here = span_of(0, u, count)
        return pltpu.make_async_remote_copy(
            rsend.at[way, t, here], rrecv.at[way, t, here], s_sem.at[0, way], r_sem(way, t, u, count),
            device_id=to[way], device_id_type=mesh_id,
        )

    def ag_send(way, t, u, count):
        c = owner(-(t // 2) if way == 0 else t // 2)
        ref = y.at[span_of(half(way, t), u, count), pl.ds(pl.multiple_of(c * cols, 128), cols)]
        return pltpu.make_async_remote_copy(
            ref, ref, s_sem.at[1, way], r_sem(way, hops + t, u, count), device_id=to[way], device_id_type=mesh_id
        )

    def own(p, h, u, count):
        here = span_of(h, u, count)
        return term[p, here] + precv[p, here].astype(F32)

    def rs_place(way, t):
        first = 1 - (t + hops - 1) // hops
        p = 2 * ((t + 1) // 2)
        return p if way else p - 1 + first

    def rs_slot(t):
        @pl.when(t == 0)
        def _():
            p_send(0).wait_recv()

        @pl.when(lax.rem(t, 2) == 1)
        def _():
            p_send(t).wait_recv()
            p_send(t + 1).wait_recv()

        def pass_on(way, u, count, add):
            total = own(rs_place(way, t), half(way, t), u, count)
            here = span_of(0, u, count)
            if add:
                total = total + rrecv[way, t - 2, here].astype(F32)
            rsend[way, t, here] = total.astype(BF16)
            rs_send(way, t, u, count).start()

        @pl.when(t < 2)
        def _():
            def begin(u):
                for way in range(2):
                    pass_on(way, u, COARSE, False)

            loop(0, COARSE, begin)

        @pl.when((t >= 2) & (t < hops - 2))
        def _():
            def middle(u):
                for way in range(2):
                    rs_send(way, t - 2, u, COARSE).wait_recv()
                    pass_on(way, u, COARSE, True)

            loop(0, COARSE, middle)

        @pl.when(t >= hops - 2)
        def _():
            def end(u):
                for way in range(2):
                    rs_send(way, t - 2, u, COARSE).wait_recv()
                    for v in range(FINE // COARSE):
                        pass_on(way, u * (FINE // COARSE) + v, FINE, True)

            loop(0, COARSE, end)

    def down_and_ring(p):
        @pl.when(p < n)
        def _():
            down(p)

        late = p // 6

        @pl.when(lax.rem(p, 2) + late >= 1)
        def _():
            rs_slot((1 - late) * ((p - 1) // 2) + late * (p - 3))

    loop(0, hops + 3, down_and_ring)
    p_send(hops).wait_recv()

    mine_y = pl.ds(pl.multiple_of(me * cols, 128), cols)

    def finish(u):
        for h in range(2):
            total = own(hops, h, u, FINE)
            for way in range(2):
                t = hops - 1 if (way + hops - 1) % 2 == h else hops - 2
                rs_send(way, t, u, FINE).wait_recv()
                total = total + rrecv[way, t, span_of(0, u, FINE)].astype(F32)
            y[span_of(h, u, FINE), mine_y] = total.astype(BF16)
            for way in (h, 1 - h):
                ag_send(way, (h + way) % 2, u, FINE).start()

    loop(0, FINE, finish)

    def forward_first(t):
        def one(u):
            for way in range(2):
                for v in range(FINE // COARSE):
                    ag_send(way, t - 2, u * (FINE // COARSE) + v, FINE).wait_recv()
                ag_send(way, t, u, COARSE).start()

        loop(0, COARSE, one)

    def forward(t):
        def one(u):
            for way in range(2):
                ag_send(way, t - 2, u, COARSE).wait_recv()
                ag_send(way, t, u, COARSE).start()

        loop(0, COARSE, one)

    loop(2, 4, forward_first)
    loop(4, hops, forward)

    def last(u):
        for t in (hops - 2, hops - 1):
            for way in range(2):
                ag_send(way, t, u, COARSE).wait_recv()

    loop(0, COARSE, last)

    pltpu.make_async_remote_copy(
        xbuf.at[pl.ds(0, rows)], xbuf.at[pl.ds(rows, rows)], xs_sem, xr_sem.at[0], device_id=partner, device_id_type=mesh_id
    ).wait_send()
    pltpu.make_async_remote_copy(
        psend, precv, ps_sem, pr_sem.at[0], device_id=partner, device_id_type=mesh_id
    ).wait_send()
    for way in range(2):
        for stage in range(2):
            pltpu.make_async_remote_copy(
                rsend.at[way], rrecv.at[way], s_sem.at[stage, way], coarse_sem.at[0, 0, 0],
                device_id=to[way], device_id_type=mesh_id,
            ).wait_send()


def solution(mesh):
    n = mesh.shape["tp"]

    def step(x, w_gate, w_up, w_down):
        rows, depth = x.shape
        share = w_gate.shape[1]
        part, cols, chunks = share // 2, depth // n, depth // CHUNK
        hops = n - 1
        dma = pltpu.SemaphoreType.DMA
        return pl.pallas_call(
            functools.partial(kernel, n),
            out_shape=pltpu.VMEM((rows, depth), BF16),
            in_specs=[pl.BlockSpec(memory_space=pl.ANY)] * 4,
            out_specs=pl.BlockSpec(memory_space=pltpu.VMEM),
            scratch_shapes=[
                pltpu.VMEM((2 * rows, depth), BF16),
                pltpu.VMEM((SLOTS, CHUNK, share), BF16),
                pltpu.VMEM((n, part, cols), BF16),
                pltpu.VMEM((2 * rows, share), F32),
                pltpu.VMEM((2 * rows, part), BF16),
                pltpu.VMEM((n, rows, cols), F32),
                pltpu.VMEM((n, rows, cols), BF16),
                pltpu.VMEM((n, rows, cols), BF16),
                pltpu.VMEM((2, hops, rows // 2, cols), BF16),
                pltpu.VMEM((2, hops, rows // 2, cols), BF16),
                dma,
                dma,
                dma((chunks,)),
                dma((chunks,)),
                dma((n,)),
                dma,
                dma((n,)),
                dma((2, 2)),
                dma((2, 4, FINE)),
                dma((2, hops - 2, COARSE)),
            ],
            compiler_params=pltpu.CompilerParams(
                collective_id=0, has_side_effects=True, vmem_limit_bytes=62 * 1024 * 1024
            ),
        )(x, w_gate, w_up, w_down)

    return jax.shard_map(
        step,
        mesh=mesh,
        in_specs=(P("dp", None), P(None, "tp"), P(None, "tp"), P("tp", None)),
        out_specs=P("dp", None),
        check_vma=False,
    )
```

```python
import functools

import jax
import jax.numpy as jnp
from jax import lax
from jax.experimental import pallas as pl
from jax.experimental.pallas import tpu as pltpu
from jax.sharding import PartitionSpec as P

F32, BF16 = jnp.float32, jnp.bfloat16
CHUNK = 1024
SLOTS = 5
FINE = 4
COARSE = 2
ACT_ROWS = 32


def kernel(n, x_hbm, wg_hbm, wu_hbm, wd_hbm, y, xbuf, wgu, wd, acc, hid, term, psend, precv, rsend, rrecv,
           x_sem, xs_sem, xr_sem, w_sem, d_sem, ps_sem, pr_sem, s_sem, fine_sem, coarse_sem):
    rows, depth = x_hbm.shape
    part = wg_hbm.shape[1] // 2
    cols = depth // n
    half_rows = rows // 2
    far = n // 2
    hops = n - 1
    chunks = depth // CHUNK

    dp, me = lax.axis_index("dp"), lax.axis_index("tp")
    side = lax.rem(dp, 2)
    partner = {"dp": dp + 1 - 2 * side}
    right, left = {"tp": lax.rem(me + 1, n)}, {"tp": lax.rem(me + n - 1, n)}
    to = (right, left)
    mesh_id = pl.DeviceIdType.MESH

    def owner(off):
        return lax.rem(me + off + n, n)

    mine = pl.ds(pl.multiple_of(side * part, 128), part)

    def span(k):
        return pl.ds(pl.multiple_of(k * CHUNK, CHUNK), CHUNK)

    x_copy = pltpu.make_async_copy(x_hbm, xbuf.at[pl.ds(0, rows)], x_sem)

    def w_copies(k):
        slot = lax.rem(k, SLOTS)
        return (
            pltpu.make_async_copy(wg_hbm.at[span(k), mine], wgu.at[slot, :, pl.ds(0, part)], w_sem.at[slot]),
            pltpu.make_async_copy(wu_hbm.at[span(k), mine], wgu.at[slot, :, pl.ds(part, part)], w_sem.at[slot]),
        )

    def w_wait(k):
        pltpu.make_async_copy(wg_hbm.at[span(k)], wgu.at[lax.rem(k, SLOTS)], w_sem.at[lax.rem(k, SLOTS)]).wait()

    def at(p):
        dist = far - (p + 1) // 2
        return owner(dist * (2 * lax.rem(p, 2) - 1))

    def d_copy(p):
        return pltpu.make_async_copy(
            wd_hbm.at[mine, pl.ds(pl.multiple_of(at(p) * cols, 128), cols)], wd.at[p], d_sem.at[p]
        )

    def start_all(*copies):
        for c in copies:
            c.start(priority=1)

    def x_send(k):
        return pltpu.make_async_remote_copy(
            xbuf.at[pl.ds(0, rows), span(k)], xbuf.at[pl.ds(rows, rows), span(k)], xs_sem, xr_sem.at[k],
            device_id=partner, device_id_type=mesh_id,
        )

    def loop(lo, hi, body):
        def run(i, carry):
            body(i)
            return carry

        lax.fori_loop(lo, hi, run, 0)

    x_copy.start()
    loop(0, SLOTS, lambda k: start_all(*w_copies(k)))

    barrier = pltpu.get_barrier_semaphore()
    for other in (left, right, partner):
        pl.semaphore_signal(barrier, inc=1, device_id=other, device_id_type=mesh_id)
    pl.semaphore_wait(barrier, 3)

    x_copy.wait()
    loop(0, chunks, lambda k: x_send(k).start())

    def zero(r):
        acc[pl.ds(pl.multiple_of(r * 16, 16), 16)] = jnp.zeros((16, 2 * part), F32)

    loop(0, 2 * rows // 16, zero)

    def gate_up(k):
        w_wait(k)
        x_send(k).wait_recv()
        acc[...] += jnp.dot(xbuf[:, span(k)], wgu[lax.rem(k, SLOTS)], preferred_element_type=F32)

        @pl.when(k + SLOTS < chunks)
        def _():
            start_all(*w_copies(k + SLOTS))

        @pl.when(k + SLOTS == chunks - 1)
        def _():
            loop(0, n, lambda p: start_all(d_copy(p)))

    loop(0, chunks, gate_up)

    def activate(r):
        here = pl.ds(pl.multiple_of(r * ACT_ROWS, ACT_ROWS), ACT_ROWS)
        hid[here] = (jax.nn.silu(acc[here, :part]) * acc[here, part:]).astype(BF16)

    loop(0, 2 * rows // ACT_ROWS, activate)

    def p_send(p):
        return pltpu.make_async_remote_copy(
            psend.at[p], precv.at[p], ps_sem, pr_sem.at[(p + 1) // 2], device_id=partner, device_id_type=mesh_id
        )

    def down(p):
        d_copy(p).wait()
        got = jnp.dot(hid[...], wd[p], preferred_element_type=F32)
        psend[p] = got[rows:].astype(BF16)
        p_send(p).start()
        term[p] = got[:rows]

    def half(way, t):
        return lax.rem(way + t, 2)

    def span_of(h, u, count):
        size = half_rows // count
        return pl.ds(pl.multiple_of(h * half_rows + u * size, size), size)

    def r_sem(way, slot, u, count):
        if count == FINE:
            return fine_sem.at[way, slot - (hops - 2), u]
        return coarse_sem.at[way, slot - (hops + 2) * (slot // (hops + 2)), u]

    def rs_send(way, t, u, count):
        here = span_of(0, u, count)
        return pltpu.make_async_remote_copy(
            rsend.at[way, t, here], rrecv.at[way, t, here], s_sem.at[0, way], r_sem(way, t, u, count),
            device_id=to[way], device_id_type=mesh_id,
        )

    def ag_send(way, t, u, count):
        c = owner(-(t // 2) if way == 0 else t // 2)
        ref = y.at[span_of(half(way, t), u, count), pl.ds(pl.multiple_of(c * cols, 128), cols)]
        return pltpu.make_async_remote_copy(
            ref, ref, s_sem.at[1, way], r_sem(way, hops + t, u, count), device_id=to[way], device_id_type=mesh_id
        )

    def own(p, h, u, count):
        here = span_of(h, u, count)
        return term[p, here] + precv[p, here].astype(F32)

    def rs_place(way, t):
        first = 1 - (t + hops - 1) // hops
        p = 2 * ((t + 1) // 2)
        return p if way else p - 1 + first

    def rs_slot(t):
        @pl.when(t == 0)
        def _():
            p_send(0).wait_recv()

        @pl.when(lax.rem(t, 2) == 1)
        def _():
            both = pl.ds(t, 2)
            pltpu.make_async_remote_copy(
                psend.at[both], precv.at[both], ps_sem, pr_sem.at[(t + 1) // 2], device_id=partner, device_id_type=mesh_id
            ).wait_recv()

        def pass_on(way, u, count, add):
            total = own(rs_place(way, t), half(way, t), u, count)
            here = span_of(0, u, count)
            if add:
                total = total + rrecv[way, t - 2, here].astype(F32)
            rsend[way, t, here] = total.astype(BF16)
            rs_send(way, t, u, count).start()

        @pl.when(t < 2)
        def _():
            def begin(u):
                for way in range(2):
                    pass_on(way, u, COARSE, False)

            loop(0, COARSE, begin)

        @pl.when((t >= 2) & (t < hops - 2))
        def _():
            def middle(u):
                for way in range(2):
                    rs_send(way, t - 2, u, COARSE).wait_recv()
                    pass_on(way, u, COARSE, True)

            loop(0, COARSE, middle)

        @pl.when(t >= hops - 2)
        def _():
            def end(u):
                for way in range(2):
                    rs_send(way, t - 2, u, COARSE).wait_recv()
                    for v in range(FINE // COARSE):
                        pass_on(way, u * (FINE // COARSE) + v, FINE, True)

            loop(0, COARSE, end)

    def down_and_ring(p):
        @pl.when(p < n)
        def _():
            down(p)

        late = p // 6

        @pl.when(lax.rem(p, 2) + late >= 1)
        def _():
            rs_slot((1 - late) * ((p - 1) // 2) + late * (p - 3))

    loop(0, hops + 3, down_and_ring)
    p_send(hops).wait_recv()

    mine_y = pl.ds(pl.multiple_of(me * cols, 128), cols)

    def finish(u):
        for h in range(2):
            total = own(hops, h, u, FINE)
            for way in range(2):
                t = hops - 1 if (way + hops - 1) % 2 == h else hops - 2
                rs_send(way, t, u, FINE).wait_recv()
                total = total + rrecv[way, t, span_of(0, u, FINE)].astype(F32)
            y[span_of(h, u, FINE), mine_y] = total.astype(BF16)
            for way in (h, 1 - h):
                ag_send(way, (h + way) % 2, u, FINE).start()

    loop(0, FINE, finish)

    def forward_first(t):
        def one(u):
            for way in range(2):
                for v in range(FINE // COARSE):
                    ag_send(way, t - 2, u * (FINE // COARSE) + v, FINE).wait_recv()
                ag_send(way, t, u, COARSE).start()

        loop(0, COARSE, one)

    def forward(t):
        def one(u):
            for way in range(2):
                ag_send(way, t - 2, u, COARSE).wait_recv()
                ag_send(way, t, u, COARSE).start()

        loop(0, COARSE, one)

    loop(2, 4, forward_first)
    loop(4, hops, forward)

    def last(u):
        for t in (hops - 2, hops - 1):
            for way in range(2):
                ag_send(way, t, u, COARSE).wait_recv()

    loop(0, COARSE, last)

    pltpu.make_async_remote_copy(
        xbuf.at[pl.ds(0, rows)], xbuf.at[pl.ds(rows, rows)], xs_sem, xr_sem.at[0], device_id=partner, device_id_type=mesh_id
    ).wait_send()
    pltpu.make_async_remote_copy(
        psend, precv, ps_sem, pr_sem.at[0], device_id=partner, device_id_type=mesh_id
    ).wait_send()
    for way in range(2):
        for stage in range(2):
            pltpu.make_async_remote_copy(
                rsend.at[way], rrecv.at[way], s_sem.at[stage, way], coarse_sem.at[0, 0, 0],
                device_id=to[way], device_id_type=mesh_id,
            ).wait_send()


def solution(mesh):
    n = mesh.shape["tp"]

    def step(x, w_gate, w_up, w_down):
        rows, depth = x.shape
        share = w_gate.shape[1]
        part, cols, chunks = share // 2, depth // n, depth // CHUNK
        hops = n - 1
        dma = pltpu.SemaphoreType.DMA
        return pl.pallas_call(
            functools.partial(kernel, n),
            out_shape=pltpu.VMEM((rows, depth), BF16),
            in_specs=[pl.BlockSpec(memory_space=pl.ANY)] * 4,
            out_specs=pl.BlockSpec(memory_space=pltpu.VMEM),
            scratch_shapes=[
                pltpu.VMEM((2 * rows, depth), BF16),
                pltpu.VMEM((SLOTS, CHUNK, share), BF16),
                pltpu.VMEM((n, part, cols), BF16),
                pltpu.VMEM((2 * rows, share), F32),
                pltpu.VMEM((2 * rows, part), BF16),
                pltpu.VMEM((n, rows, cols), F32),
                pltpu.VMEM((n, rows, cols), BF16),
                pltpu.VMEM((n, rows, cols), BF16),
                pltpu.VMEM((2, hops, rows // 2, cols), BF16),
                pltpu.VMEM((2, hops, rows // 2, cols), BF16),
                dma,
                dma,
                dma((chunks,)),
                dma((SLOTS,)),
                dma((n,)),
                dma,
                dma((n // 2 + 1,)),
                dma((2, 2)),
                dma((2, 4, FINE)),
                dma((2, hops - 2, COARSE)),
            ],
            compiler_params=pltpu.CompilerParams(
                collective_id=0, has_side_effects=True, vmem_limit_bytes=62 * 1024 * 1024
            ),
        )(x, w_gate, w_up, w_down)

    return jax.shard_map(
        step,
        mesh=mesh,
        in_specs=(P("dp", None), P(None, "tp"), P(None, "tp"), P("tp", None)),
        out_specs=P("dp", None),
        check_vma=False,
    )
```
